32 devices in a mesh: dp: 2 (over x), pp: 4 (over z), ep: 4 (over y, core).
Axes of the slice: x: 2, y: 2, z: 4, core: 2. Of those that a mesh axis runs over, the one named last changes fastest.
Arguments:
- hidden_in: bfloat16 [24, 128, 1024], P(None, ('dp', 'ep')), parts along dimension 1
- seq_pos: int32 [24, 128], P(None, ('dp', 'ep')), parts along dimension 1
- k_cache: bfloat16 [4, 24, 128, 16, 8, 64], P('pp', None, ('dp', 'ep')), parts along dimension 2
- v_cache: bfloat16 [4, 24, 128, 16, 8, 64], P('pp', None, ('dp', 'ep')), parts along dimension 2
- expert_ids: int32 [4, 24, 128, 8], P('pp', None, ('dp', 'ep')), parts along dimension 2
- w_query: bfloat16 [4, 1024, 1024], P('pp')
- w_key: bfloat16 [4, 1024, 512], P('pp')
- w_value: bfloat16 [4, 1024, 512], P('pp')
- w_out: bfloat16 [4, 1024, 1024], P('pp')
- attn_gain: bfloat16 [4, 1024], P('pp')
- mlp_gain: bfloat16 [4, 1024], P('pp')
- w_router: bfloat16 [4, 1024, 32], P('pp')
- w_gate: bfloat16 [4, 32, 1024, 512], P('pp', 'ep')
- w_up: bfloat16 [4, 32, 1024, 512], P('pp', 'ep')
- w_down: bfloat16 [4, 32, 512, 1024], P('pp', 'ep')
- final_gain: bfloat16 [1024], replicated
Outputs:
- output 1: bfloat16 [24, 128, 1024], P(None, ('dp', 'ep')), parts along dimension 1
- output 2: bfloat16 [4, 24, 128, 8, 64], P('pp', None, ('dp', 'ep')), parts along dimension 2
- output 3: bfloat16 [4, 24, 128, 8, 64], P('pp', None, ('dp', 'ep')), parts along dimension 2
There are 2 independent parts. The reference program is written for one: setup_inputs(seed, part) draws one part's arguments, and reference() takes and returns one part's arrays. A program takes and returns all parts, laid end to end along the dimension named above; an argument that names none is the same for every part.
All inputs are finite; a program needn't handle non-finite values.
Results may differ from the reference program's by a relative error of at most 0.02.
Values are sent between devices in bfloat16 or wider.
A program may use at most 1 GiB of HBM per device.

```python
import jax
import jax.numpy as jnp
from jax import lax

D = 1024
HEADS = 16
KV_HEADS = 8
HEAD = 64
EXPERTS = 32
FF = 512
TOP = 8
LAYERS = 4
EP_SIZE = 4
MICRO_COUNT = 24
TOK_DEV = 16
CONTEXT = 16
MICRO_ROWS = EP_SIZE * TOK_DEV
LOCAL_EXPERTS = EXPERTS // EP_SIZE
THETA = 1000000.0
EPS = 1e-05


def draw_routes(route_key):
    hot_key, perm_key, local_key = jax.random.split(route_key, 3)
    hot_dev = jax.random.randint(hot_key, (LAYERS, MICRO_COUNT, 1, 1), 0, EP_SIZE)
    perm_keys = jax.random.split(perm_key, LAYERS * MICRO_COUNT * EP_SIZE)
    slot_pos = jax.vmap(lambda one_key: jax.random.permutation(one_key, TOK_DEV))(perm_keys)
    slot_pos = slot_pos.reshape(LAYERS, MICRO_COUNT, EP_SIZE, TOK_DEV)
    first_dev = jnp.where(slot_pos < TOK_DEV // 2, hot_dev, (hot_dev + slot_pos) % EP_SIZE)
    local_base = jax.random.randint(local_key, (LAYERS, MICRO_COUNT, EP_SIZE, TOK_DEV, 1), 0, LOCAL_EXPERTS)
    choice = jnp.arange(TOP)
    dest_dev = (first_dev[..., None] + choice) % EP_SIZE
    local_idx = (local_base + choice // EP_SIZE) % LOCAL_EXPERTS
    route_ids = dest_dev * LOCAL_EXPERTS + local_idx
    return route_ids.reshape(LAYERS, MICRO_COUNT, MICRO_ROWS, TOP).astype(jnp.int32)


def draw_normal(one_key, arr_shape, std_scale):
    return (jax.random.normal(one_key, arr_shape, jnp.float32) * std_scale).astype(jnp.bfloat16)


def draw_gain(one_key, arr_shape):
    return (1.0 + 0.3 * jax.random.normal(one_key, arr_shape, jnp.float32)).astype(jnp.bfloat16)


def setup_inputs(seed: int = 0, part: int = 0) -> dict:
    shared_keys = jax.random.split(jax.random.key(seed), 11)
    part_keys = jax.random.split(jax.random.fold_in(jax.random.key(seed + 1), part), 5)
    pos_draw = jax.random.randint(part_keys[1], (MICRO_COUNT, MICRO_ROWS), 1, CONTEXT + 1)
    first_row = jnp.arange(MICRO_COUNT * MICRO_ROWS).reshape(MICRO_COUNT, MICRO_ROWS) == 0
    seq_pos = jnp.where(first_row, CONTEXT, pos_draw).astype(jnp.int32)
    cache_shape = (LAYERS, MICRO_COUNT, MICRO_ROWS, CONTEXT, KV_HEADS, HEAD)
    out_scale = 0.5 * (CONTEXT ** 0.5) * (HEADS * HEAD) ** -0.5
    return {
        "hidden_in": draw_normal(part_keys[0], (MICRO_COUNT, MICRO_ROWS, D), 1.0),
        "seq_pos": seq_pos,
        "k_cache": draw_normal(part_keys[2], cache_shape, 1.0),
        "v_cache": draw_normal(part_keys[3], cache_shape, 1.0),
        "expert_ids": draw_routes(part_keys[4]),
        "w_query": draw_normal(shared_keys[0], (LAYERS, D, HEADS * HEAD), D ** -0.5),
        "w_key": draw_normal(shared_keys[1], (LAYERS, D, KV_HEADS * HEAD), D ** -0.5),
        "w_value": draw_normal(shared_keys[2], (LAYERS, D, KV_HEADS * HEAD), D ** -0.5),
        "w_out": draw_normal(shared_keys[3], (LAYERS, HEADS * HEAD, D), out_scale),
        "attn_gain": draw_gain(shared_keys[4], (LAYERS, D)),
        "mlp_gain": draw_gain(shared_keys[5], (LAYERS, D)),
        "w_router": draw_normal(shared_keys[6], (LAYERS, D, EXPERTS), 2.0 * D ** -0.5),
        "w_gate": draw_normal(shared_keys[7], (LAYERS, EXPERTS, D, FF), D ** -0.5),
        "w_up": draw_normal(shared_keys[8], (LAYERS, EXPERTS, D, FF), D ** -0.5),
        "w_down": draw_normal(shared_keys[9], (LAYERS, EXPERTS, FF, D), FF ** -0.5),
        "final_gain": draw_gain(shared_keys[10], (D,)),
    }


def rms_norm(in_vals, gain_vec):
    vals_f32 = in_vals.astype(jnp.float32)
    inv_rms = lax.rsqrt(jnp.mean(vals_f32 * vals_f32, axis=-1, keepdims=True) + EPS)
    return (vals_f32 * inv_rms * gain_vec.astype(jnp.float32)).astype(jnp.bfloat16)


def rotate(head_vecs, positions):
    half_dim = head_vecs.shape[-1] // 2
    inv_freq = THETA ** (-jnp.arange(half_dim, dtype=jnp.float32) / half_dim)
    angles = positions.astype(jnp.float32)[:, None, None] * inv_freq
    cos_ang = jnp.cos(angles)
    sin_ang = jnp.sin(angles)
    first_half = head_vecs[..., :half_dim].astype(jnp.float32)
    second_half = head_vecs[..., half_dim:].astype(jnp.float32)
    return jnp.concatenate([first_half * cos_ang - second_half * sin_ang, second_half * cos_ang + first_half * sin_ang], axis=-1).astype(jnp.bfloat16)


def attend(q_heads, key_new, val_new, k_rows, v_rows, positions):
    tokens = key_new.shape[0]
    q_groups = q_heads.reshape(tokens, KV_HEADS, HEADS // KV_HEADS, HEAD).astype(jnp.float32)
    score_scale = HEAD ** -0.5
    cache_scores = jnp.einsum("bkgh,btkh->bkgt", q_groups, k_rows.astype(jnp.float32)) * score_scale
    is_valid = jnp.arange(CONTEXT)[None, None, None, :] < positions[:, None, None, None]
    cache_scores = jnp.where(is_valid, cache_scores, -jnp.inf)
    self_score = jnp.einsum("bkgh,bkh->bkg", q_groups, key_new.astype(jnp.float32))[..., None] * score_scale
    top_score = jnp.maximum(jnp.max(cache_scores, axis=-1, keepdims=True), self_score)
    cache_w = jnp.exp(cache_scores - top_score)
    self_w = jnp.exp(self_score - top_score)
    weight_sum = jnp.sum(cache_w, axis=-1, keepdims=True) + self_w
    cache_w = (cache_w / weight_sum).astype(jnp.bfloat16).astype(jnp.float32)
    self_w = (self_w / weight_sum).astype(jnp.bfloat16).astype(jnp.float32)
    attn_out = jnp.einsum("bkgt,btkh->bkgh", cache_w, v_rows.astype(jnp.float32)) + self_w * val_new.astype(jnp.float32)[:, :, None, :]
    return attn_out.astype(jnp.bfloat16).reshape(tokens, HEADS * HEAD)


def one_micro(hidden, positions, k_rows, v_rows, choice_ids, layer_w):
    w_q, w_k, w_v, w_o, a_gain, m_gain, w_r, w_g, w_u, w_d = layer_w
    tokens = hidden.shape[0]
    normed = rms_norm(hidden, a_gain)
    q_heads = jnp.dot(normed, w_q, preferred_element_type=jnp.float32).astype(jnp.bfloat16).reshape(tokens, HEADS, HEAD)
    key_new = jnp.dot(normed, w_k, preferred_element_type=jnp.float32).astype(jnp.bfloat16).reshape(tokens, KV_HEADS, HEAD)
    val_new = jnp.dot(normed, w_v, preferred_element_type=jnp.float32).astype(jnp.bfloat16).reshape(tokens, KV_HEADS, HEAD)
    q_heads = rotate(q_heads, positions)
    key_new = rotate(key_new, positions)
    attn_out = attend(q_heads, key_new, val_new, k_rows, v_rows, positions)
    hidden = (hidden.astype(jnp.float32) + jnp.dot(attn_out, w_o, preferred_element_type=jnp.float32)).astype(jnp.bfloat16)
    normed = rms_norm(hidden, m_gain)
    logits = jnp.dot(normed, w_r, preferred_element_type=jnp.float32)
    gate_vals = jax.nn.softmax(jnp.take_along_axis(logits, choice_ids, axis=1), axis=-1)
    coef_mat = jnp.sum(gate_vals[:, :, None] * (choice_ids[:, :, None] == jnp.arange(EXPERTS)[None, None, :]), axis=1)

    def expert_body(acc_sum, expert_args):
        gate_w, up_w, down_w, coef_col = expert_args
        act_rows = (jax.nn.silu(jnp.dot(normed, gate_w, preferred_element_type=jnp.float32)) * jnp.dot(normed, up_w, preferred_element_type=jnp.float32)).astype(jnp.bfloat16)
        down_h = jnp.dot(act_rows, down_w, preferred_element_type=jnp.float32)
        return acc_sum + (coef_col[:, None] * down_h).astype(jnp.bfloat16).astype(jnp.float32), None

    moe_sum, _ = lax.scan(expert_body, jnp.zeros(hidden.shape, jnp.float32), (w_g, w_u, w_d, coef_mat.T))
    hidden = (hidden.astype(jnp.float32) + moe_sum.astype(jnp.bfloat16).astype(jnp.float32)).astype(jnp.bfloat16)
    return hidden, key_new, val_new


def reference(hidden_in, seq_pos, k_cache, v_cache, expert_ids, w_query, w_key, w_value, w_out, attn_gain, mlp_gain, w_router, w_gate, w_up, w_down, final_gain):
    def layer_body(hidden, layer_args):
        layer_w = layer_args[3:]

        def micro_body(micro_args):
            return one_micro(micro_args[0], micro_args[1], micro_args[2], micro_args[3], micro_args[4], layer_w)

        hidden, k_rows, v_rows = lax.map(micro_body, (hidden, seq_pos, layer_args[0], layer_args[1], layer_args[2]))
        return hidden, (k_rows, v_rows)

    hidden, new_rows = lax.scan(layer_body, hidden_in, (k_cache, v_cache, expert_ids, w_query, w_key, w_value, w_out, attn_gain, mlp_gain, w_router, w_gate, w_up, w_down))
    return rms_norm(hidden, final_gain), new_rows[0], new_rows[1]
```

```python
import functools

import jax
import jax.numpy as jnp
from jax import lax
from jax.experimental import pallas as pl
from jax.experimental.pallas import tpu as pltpu
from jax.sharding import PartitionSpec as P

THETA = 1000000.0
EPS = 1e-05
MICRO_PER_CHUNK = 2
MESH = pl.DeviceIdType.MESH
F32 = jnp.float32
BF16 = jnp.bfloat16


def rms(vals, gain):
    inv = lax.rsqrt(jnp.mean(vals * vals, axis=-1, keepdims=True) + EPS)
    return (vals * inv * gain).astype(BF16)


def dot(lhs, rhs):
    return jnp.dot(lhs, rhs, preferred_element_type=F32)


def dot_t(lhs, rhs):
    return lax.dot_general(lhs, rhs, (((1,), (1,)), ((), ())), preferred_element_type=F32)


def rounded(vals):
    return vals.astype(BF16).astype(F32)


def stack_kernel(cfg, hid_hbm, k_hbm, v_hbm, wq_hbm, wk_hbm, wv_hbm, wo_hbm, wg_hbm, wu_hbm, wd_hbm, cos_ref, sin_ref, tm_ref, mh_ref, ag_ref, mg_ref, fg_ref, wr_ref, out_ref, ko_ref, vo_ref, wq, wk, wv, wo, wg, wu, wd, h_in, h_mid, h_out, n_all, part, rs_sib, rs_cp, kbuf, vbuf, q2, k2, v2, o2, kn, act, coef, w_sem, kv_sem, hid_sem, ag_send, ag_recv, rs_send, rs_recv, pp_send, pp_recv, bc_send, bc_recv):
    chunks, rows, stages = cfg
    every = 4 * rows
    stage = lax.axis_index("pp")
    me = lax.axis_index("ep")
    sib = me + 1 - 2 * lax.rem(me, 2)
    cp = lax.rem(me + 2, 4)
    diag = lax.rem(sib + 2, 4)
    last = stages - 1

    def block(dev):
        return pl.ds(pl.multiple_of(dev * rows, rows), rows)

    attn_w = [pltpu.make_async_copy(src, dst, w_sem.at[i]) for i, (src, dst) in enumerate(((wq_hbm, wq), (wk_hbm, wk), (wv_hbm, wv), (wo_hbm, wo)))]
    moe_w = [pltpu.make_async_copy(src, dst, w_sem.at[i + 4]) for i, (src, dst) in enumerate(((wg_hbm, wg), (wu_hbm, wu), (wd_hbm, wd)))]

    def kv_copies(c):
        slot = lax.rem(c, 2)
        span = pl.ds(pl.multiple_of(c * rows * 128, rows * 128), rows * 128)
        return (pltpu.make_async_copy(k_hbm.at[span], kbuf.at[slot], kv_sem.at[0, slot]), pltpu.make_async_copy(v_hbm.at[span], vbuf.at[slot], kv_sem.at[1, slot]))

    hid_copy = pltpu.make_async_copy(hid_hbm, h_in, hid_sem)

    @pl.when(stage == 0)
    def _():
        hid_copy.start()

    for copy in attn_w:
        copy.start()
    for copy in kv_copies(0):
        copy.start()

    barrier = pltpu.get_barrier_semaphore()
    pl.semaphore_signal(barrier, inc=1, device_id={"ep": sib}, device_id_type=MESH)
    pl.semaphore_signal(barrier, inc=1, device_id={"ep": cp}, device_id_type=MESH)
    for step in range(1, stages):
        pl.semaphore_signal(barrier, inc=1, device_id={"pp": lax.rem(stage + step, stages)}, device_id_type=MESH)
    pl.semaphore_wait(barrier, 2 + stages - 1)

    def ag_copy(which, c):
        src = n_all.at[c, block(cp if which == 2 else me)]
        target = cp if which == 1 else sib
        return pltpu.make_async_remote_copy(src, src, ag_send.at[which, c], ag_recv.at[which, c], device_id={"ep": target}, device_id_type=MESH)

    def rs_copy(which, c):
        slot = lax.rem(c, 2)
        src = part.at[slot, block((sib, diag, cp)[which])]
        dst = rs_cp.at[c] if which == 2 else rs_sib.at[which, c]
        target = cp if which == 2 else sib
        return pltpu.make_async_remote_copy(src, dst, rs_send.at[which, c], rs_recv.at[which, c], device_id={"ep": target}, device_id_type=MESH)

    def pp_copy(c):
        return pltpu.make_async_remote_copy(h_out.at[c], h_in.at[c], pp_send.at[c], pp_recv.at[c], device_id={"pp": lax.rem(stage + 1, stages)}, device_id_type=MESH)

    def bc_copy(c, target):
        return pltpu.make_async_remote_copy(out_ref.at[c], out_ref.at[c], bc_send.at[target, c], bc_recv.at[c], device_id={"pp": target}, device_id_type=MESH)

    lane = lax.broadcasted_iota(jnp.int32, (rows, 128), 1)
    low_half = lane < 64
    first_part = lax.rem(lane, 64) < 32
    own_head = lax.rem(lax.broadcasted_iota(jnp.int32, (16, 128), 1), 8) == lax.broadcasted_iota(jnp.int32, (16, 128), 0) // 2

    def rope(vals, cos, sin):
        turned = jnp.where(first_part, pltpu.roll(vals, 96, 1), pltpu.roll(vals, 32, 1))
        return rounded(vals * cos + turned * sin)

    def attend(c):
        slot = lax.rem(c, 2)

        @pl.when(stage > 0)
        def _():
            pp_copy(c).wait_recv()

        @pl.when((stage == 0) & (c == 0))
        def _():
            hid_copy.wait()

        @pl.when(c == 0)
        def _():
            for copy in attn_w:
                copy.wait()
            for copy in moe_w:
                copy.start()

        @pl.when(c + 1 < chunks)
        def _():
            for copy in kv_copies(c + 1):
                copy.start()

        span = pl.ds(pl.multiple_of(c * rows, rows), rows)
        cos = cos_ref[span, :]
        sin = sin_ref[span, :]
        hidden = h_in[c].astype(F32)
        normed = rms(hidden, ag_ref[...])
        query = rounded(dot(normed, wq[...]))
        key = rounded(dot(normed, wk[...]))
        value = rounded(dot(normed, wv[...]))
        for j in range(8):
            piece = rope(query[:, j * 128:(j + 1) * 128], cos, sin)
            q2[pl.ds(2 * j, rows, stride=16), :] = piece
            q2[pl.ds(2 * j + 1, rows, stride=16), :] = pltpu.roll(piece, 64, 1)
        for which, full in ((0, key), (1, value)):
            spread = (k2, v2)[which]
            for j in range(4):
                piece = full[:, j * 128:(j + 1) * 128]
                if which == 0:
                    piece = rope(piece, cos, sin)
                other = pltpu.roll(piece, 64, 1)
                kn[which, pl.ds(2 * j, rows, stride=8), :] = piece
                kn[which, pl.ds(2 * j + 1, rows, stride=8), :] = other
                spread[pl.ds(4 * j, rows, stride=16), :] = piece
                spread[pl.ds(4 * j + 1, rows, stride=16), :] = piece
                spread[pl.ds(4 * j + 2, rows, stride=16), :] = other
                spread[pl.ds(4 * j + 3, rows, stride=16), :] = other
        new_span = pl.ds(pl.multiple_of(c * rows * 8, rows * 8), rows * 8)
        ko_ref[new_span, :] = kn[0, :, :64].astype(BF16)
        vo_ref[new_span, :] = kn[1, :, :64].astype(BF16)
        for copy in kv_copies(c):
            copy.wait()

        @pl.loop(0, rows // 8)
        def _(g):
            heads = pl.ds(pl.multiple_of(g * 128, 128), 128)
            q_f32 = q2[heads, :64]
            q_bf = q_f32.astype(BF16)
            scores = []
            for b in range(8):
                keys = kbuf[slot, pl.ds(pl.multiple_of((g * 8 + b) * 128, 128), 128), :]
                valid = tm_ref[pl.ds(c * rows + g * 8 + b, 1), :] > 0
                one = dot_t(q_bf[b * 16:(b + 1) * 16], keys) * 0.125
                scores.append(jnp.where(own_head & valid, one, -jnp.inf))
            score = jnp.concatenate(scores, axis=0)
            self_score = jnp.sum(q_f32 * k2[heads, :64], axis=1, keepdims=True) * 0.125
            top = jnp.maximum(jnp.max(score, axis=1, keepdims=True), self_score)
            weight = jnp.exp(score - top)
            self_w = jnp.exp(self_score - top)
            total = jnp.sum(weight, axis=1, keepdims=True) + self_w
            weight = (weight / total).astype(BF16)
            self_w = rounded(self_w / total)
            outs = []
            for b in range(8):
                vals = vbuf[slot, pl.ds(pl.multiple_of((g * 8 + b) * 128, 128), 128), :]
                outs.append(dot(weight[b * 16:(b + 1) * 16], vals))
            mixed = jnp.concatenate(outs, axis=0) + self_w * v2[heads, :64]
            o2[heads, :64] = mixed

        pieces = []
        for j in range(8):
            even = o2[pl.ds(2 * j, rows, stride=16), :]
            odd = o2[pl.ds(2 * j + 1, rows, stride=16), :]
            pieces.append(jnp.where(low_half, even, pltpu.roll(odd, 64, 1)).astype(BF16))
        attn_out = jnp.concatenate(pieces, axis=1)
        mid = (hidden + dot(attn_out, wo[...])).astype(BF16)
        h_mid[c] = mid
        n_all[c, block(me), :] = rms(mid.astype(F32), mg_ref[...])
        ag_copy(1, c).start()
        ag_copy(0, c).start()

    def gates(c):
        logits = dot_t(n_all[c], wr_ref[...])
        chosen = mh_ref[pl.ds(pl.multiple_of(c * every, every), every), :] > 0
        logits = jnp.where(chosen, logits, -jnp.inf)
        grown = jnp.exp(logits - jnp.max(logits, axis=1, keepdims=True))
        coef[...] = grown / jnp.sum(grown, axis=1, keepdims=True)

    def experts(c, first, count):
        slot = lax.rem(c, 2)
        expert_lane = lax.broadcasted_iota(jnp.int32, (every, 32), 1)

        @pl.loop(first, first + count)
        def _(j):
            for f in range(2):
                cols = slice(f * 256, (f + 1) * 256)
                gate_h = dot(n_all[c], wg[j, :, cols])
                up_h = dot(n_all[c], wu[j, :, cols])
                act[:, cols] = (gate_h / (1.0 + jnp.exp(-gate_h)) * up_h).astype(BF16)
            col = jnp.sum(jnp.where(expert_lane == me * 8 + j, coef[...], 0.0), axis=1, keepdims=True)
            for f in range(4):
                cols = slice(f * 256, (f + 1) * 256)
                down = dot(act[...], wd[j, :, cols])
                part[slot, :, cols] += rounded(col * down)

    @pl.loop(0, chunks + 2)
    def _(i):
        @pl.when(i < chunks)
        def _():
            attend(i)

        @pl.when(i >= 2)
        def _():
            c = i - 2
            slot = lax.rem(c, 2)
            rs_copy(0, c).wait_recv()
            rs_copy(1, c).wait_recv()
            part[slot, block(cp), :] += rs_sib[1, c]
            rs_copy(2, c).start()

        has_moe = (i >= 1) & (i <= chunks)

        @pl.when(has_moe)
        def _():
            c = i - 1

            @pl.when(c == 0)
            def _():
                for copy in moe_w:
                    copy.wait()

            @pl.when(c >= 2)
            def _():
                for which in range(3):
                    rs_copy(which, c - 2).wait_send()

            part[lax.rem(c, 2)] = jnp.zeros((every, part.shape[2]), F32)
            ag_copy(0, c).wait_recv()
            ag_copy(2, c).wait_recv()
            gates(c)
            experts(c, 0, 4)

        @pl.when(i < chunks)
        def _():
            ag_copy(1, i).wait_recv()
            ag_copy(2, i).start()

        @pl.when(has_moe)
        def _():
            c = i - 1
            experts(c, 4, 4)
            rs_copy(1, c).start()
            rs_copy(0, c).start()

        @pl.when(i >= 2)
        def _():
            c = i - 2
            slot = lax.rem(c, 2)
            rs_copy(2, c).wait_recv()
            total = part[slot, block(me), :] + rs_sib[0, c] + rs_cp[c]
            result = (h_mid[c].astype(F32) + rounded(total)).astype(BF16)

            @pl.when(stage < last)
            def _():
                h_out[c] = result
                pp_copy(c).start()

            @pl.when(stage == last)
            def _():
                out_ref[c] = rms(result.astype(F32), fg_ref[...])
                for target in range(last):
                    bc_copy(c, target).start()

    for which in range(3):
        rs_copy(which, chunks - 2).wait_send()
        rs_copy(which, chunks - 1).wait_send()

    @pl.loop(0, chunks)
    def _(c):
        for which in range(3):
            ag_copy(which, c).wait_send()

        @pl.when(stage < last)
        def _():
            pp_copy(c).wait_send()
            bc_copy(c, 0).wait_recv()

        @pl.when(stage == last)
        def _():
            for target in range(last):
                bc_copy(c, target).wait_send()


def run_stack(cfg, hidden, k_rows, v_rows, weights, cos, sin, time_mask, multi_hot, gains, router):
    chunks, rows, stages = cfg
    every = 4 * rows
    width = hidden.shape[-1]
    w_q, w_k, w_v, w_o, w_g, w_u, w_d = weights
    vmem = pl.BlockSpec(memory_space=pltpu.VMEM)
    hbm = pl.BlockSpec(memory_space=pl.ANY)
    dma = pltpu.SemaphoreType.DMA
    new_shape = jax.ShapeDtypeStruct((chunks * rows * 8, 64), BF16)
    return pl.pallas_call(
        functools.partial(stack_kernel, cfg),
        out_shape=(jax.ShapeDtypeStruct((chunks, rows, width), BF16), new_shape, new_shape),
        in_specs=[hbm] * 10 + [vmem] * 8,
        out_specs=(vmem, vmem, vmem),
        scratch_shapes=[
            pltpu.VMEM(w_q.shape, BF16),
            pltpu.VMEM(w_k.shape, BF16),
            pltpu.VMEM(w_v.shape, BF16),
            pltpu.VMEM(w_o.shape, BF16),
            pltpu.VMEM(w_g.shape, BF16),
            pltpu.VMEM(w_u.shape, BF16),
            pltpu.VMEM(w_d.shape, BF16),
            pltpu.VMEM((chunks, rows, width), BF16),
            pltpu.VMEM((chunks, rows, width), BF16),
            pltpu.VMEM((chunks, rows, width), BF16),
            pltpu.VMEM((chunks, every, width), BF16),
            pltpu.VMEM((2, every, width), F32),
            pltpu.VMEM((2, chunks, rows, width), F32),
            pltpu.VMEM((chunks, rows, width), F32),
            pltpu.VMEM((2, rows * 128, 64), BF16),
            pltpu.VMEM((2, rows * 128, 64), BF16),
            pltpu.VMEM((rows * 16, 128), F32),
            pltpu.VMEM((rows * 16, 128), F32),
            pltpu.VMEM((rows * 16, 128), F32),
            pltpu.VMEM((rows * 16, 128), F32),
            pltpu.VMEM((2, rows * 8, 128), F32),
            pltpu.VMEM((every, w_g.shape[2]), BF16),
            pltpu.VMEM((every, 32), F32),
            dma((7,)),
            dma((2, 2)),
            dma,
            dma((3, chunks)),
            dma((3, chunks)),
            dma((3, chunks)),
            dma((3, chunks)),
            dma((chunks,)),
            dma((chunks,)),
            dma((3, chunks)),
            dma((chunks,)),
        ],
        compiler_params=pltpu.CompilerParams(collective_id=0, has_side_effects=True, vmem_limit_bytes=67043328),
    )(hidden, k_rows, v_rows, w_q, w_k, w_v, w_o, w_g, w_u, w_d, cos, sin, time_mask, multi_hot, *gains, router)


def solution(mesh):
    stages = mesh.shape["pp"]
    rows_spec = ("dp", "ep")
    three_dim = P("pp", None, None)
    two_dim = P("pp", None)
    expert_spec = P("pp", "ep", None, None)
    cache_spec = P("pp", None, rows_spec, None, None, None)
    new_spec = P("pp", None, rows_spec, None, None)
    in_specs = (P(None, rows_spec, None), P(None, rows_spec), cache_spec, cache_spec, P("pp", None, rows_spec, None), three_dim, three_dim, three_dim, three_dim, two_dim, two_dim, three_dim, expert_spec, expert_spec, expert_spec, P(None))
    out_specs = (P(None, rows_spec, None), new_spec, new_spec)

    def device_fn(hidden_in, seq_pos, k_cache, v_cache, expert_ids, w_query, w_key, w_value, w_out, attn_gain, mlp_gain, w_router, w_gate, w_up, w_down, final_gain):
        micro, tokens, width = hidden_in.shape
        rows = MICRO_PER_CHUNK * tokens
        chunks = micro // MICRO_PER_CHUNK
        pos = seq_pos.reshape(micro * tokens, 1)
        lanes = jnp.arange(128)
        half = 32
        inv_freq = THETA ** (-jnp.arange(half, dtype=F32) / half)
        angles = pos.astype(F32) * jnp.tile(inv_freq, 4)[None, :]
        cos = jnp.cos(angles)
        sin = jnp.where(lanes % 64 < 32, -1.0, 1.0) * jnp.sin(angles)
        time_mask = (lanes[None, :] // 8 < pos).astype(F32)
        ids = lax.all_gather(expert_ids[0], "ep", axis=0)
        ids = ids.reshape(4, chunks, rows, 8).transpose(1, 0, 2, 3).reshape(chunks * 4 * rows, 8)
        multi_hot = jnp.sum((ids[:, :, None] == jnp.arange(32)[None, None, :]).astype(F32), axis=1)
        gains = (attn_gain.astype(F32), mlp_gain.astype(F32), final_gain.astype(F32).reshape(1, width))
        weights = (w_query[0], w_key[0], w_value[0], w_out[0], w_gate[0], w_up[0], w_down[0])
        out, k_new, v_new = run_stack((chunks, rows, stages), hidden_in.reshape(chunks, rows, width), k_cache.reshape(-1, 64), v_cache.reshape(-1, 64), weights, cos, sin, time_mask, multi_hot, gains, w_router[0].T)
        new_shape = k_cache.shape[:3] + k_cache.shape[4:]
        return out.reshape(hidden_in.shape), k_new.reshape(new_shape), v_new.reshape(new_shape)

    return jax.shard_map(device_fn, mesh=mesh, in_specs=in_specs, out_specs=out_specs, check_vma=False)
```

```python
import functools

import jax
import jax.numpy as jnp
import numpy as np
from jax import lax
from jax.experimental import pallas as pl
from jax.experimental.pallas import tpu as pltpu
from jax.sharding import PartitionSpec as P

THETA = 1000000.0
EPS = 1e-05
MICRO_PER_CHUNK = 2
UNROLL = 4
MESH = pl.DeviceIdType.MESH
F32 = jnp.float32
BF16 = jnp.bfloat16


def rms(vals, gain):
    inv = lax.rsqrt(jnp.mean(vals * vals, axis=-1, keepdims=True) + EPS)
    return (vals * inv * gain.astype(F32)).astype(BF16)


def dot(lhs, rhs):
    return jnp.dot(lhs, rhs, preferred_element_type=F32)


def dot_t(lhs, rhs):
    return lax.dot_general(lhs, rhs, (((1,), (1,)), ((), ())), preferred_element_type=F32)


def rounded(vals):
    return vals.astype(BF16).astype(F32)


def stack_kernel(cfg, hid_hbm, k_hbm, v_hbm, wq_hbm, wk_hbm, wv_hbm, wo_hbm, wg_hbm, wu_hbm, wd_hbm, rot_ref, pos_ref, ids_ref, ag_ref, mg_ref, fg_ref, wr_ref, out_ref, ko_ref, vo_ref, wq, wk, wv, wo, wg, wu, wd, h_in, h_mid, h_out, n_all, part, rs_sib, rs_cp, kbuf, vbuf, q2, k2, v2, o2, kn, act_even, act_odd, coef, pos_col, bits, w_sem, kv_sem, hid_sem, bit_send, bit_recv, ag_send, ag_recv, rs_send, rs_recv, pp_send, pp_recv, bc_send, bc_recv):
    chunks, rows, stages = cfg
    every = 4 * rows
    stage = lax.axis_index("pp")
    me = lax.axis_index("ep")
    sib = me + 1 - 2 * lax.rem(me, 2)
    cp = lax.rem(me + 2, 4)
    diag = lax.rem(sib + 2, 4)
    last = stages - 1

    def block(dev):
        return pl.ds(pl.multiple_of(dev * rows, rows), rows)

    attn_w = [pltpu.make_async_copy(src, dst, w_sem.at[i]) for i, (src, dst) in enumerate(((wq_hbm, wq), (wk_hbm, wk), (wv_hbm, wv), (wo_hbm, wo)))]
    def expert_w(j):
        return [pltpu.make_async_copy(src.at[j], dst.at[j], w_sem.at[4 + which * 8 + j]) for which, (src, dst) in enumerate(((wg_hbm, wg), (wu_hbm, wu), (wd_hbm, wd)))]

    def kv_copies(c):
        slot = lax.rem(c, 2)
        span = pl.ds(pl.multiple_of(c * rows * 128, rows * 128), rows * 128)
        return (pltpu.make_async_copy(k_hbm.at[span], kbuf.at[slot], kv_sem.at[0, slot]), pltpu.make_async_copy(v_hbm.at[span], vbuf.at[slot], kv_sem.at[1, slot]))

    hid_copy = pltpu.make_async_copy(hid_hbm, h_in, hid_sem)

    @pl.when(stage == 0)
    def _():
        hid_copy.start()

    for copy in attn_w:
        copy.start()
    for copy in kv_copies(0):
        copy.start()

    barrier = pltpu.get_barrier_semaphore()
    pl.semaphore_signal(barrier, inc=1, device_id={"ep": sib}, device_id_type=MESH)
    pl.semaphore_signal(barrier, inc=1, device_id={"ep": cp}, device_id_type=MESH)
    pl.semaphore_signal(barrier, inc=1, device_id={"ep": diag}, device_id_type=MESH)
    for step in range(1, stages):
        pl.semaphore_signal(barrier, inc=1, device_id={"pp": lax.rem(stage + step, stages)}, device_id_type=MESH)

    marks = jnp.zeros((16, ids_ref.shape[2]), jnp.int32)
    for k in range(8):
        marks = marks | lax.shift_left(jnp.int32(1), ids_ref[:, k, :])
    micro = marks.shape[1]
    bits[me, 0, :, :micro] = (marks & 65535).astype(F32)
    bits[me, 1, :, :micro] = (lax.shift_right_logical(marks, jnp.int32(16)) & 65535).astype(F32)
    pl.semaphore_wait(barrier, 3 + stages - 1)

    def bit_copy(which):
        return pltpu.make_async_remote_copy(bits.at[me], bits.at[me], bit_send.at[which], bit_recv.at[which], device_id={"ep": (sib, cp, diag)[which]}, device_id_type=MESH)

    for which in range(3):
        bit_copy(which).start()

    def ag_copy(which, c):
        src = n_all.at[c, block(cp if which == 2 else me)]
        target = cp if which == 1 else sib
        return pltpu.make_async_remote_copy(src, src, ag_send.at[which, c], ag_recv.at[which, c], device_id={"ep": target}, device_id_type=MESH)

    def rs_copy(which, c):
        slot = lax.rem(c, 2)
        src = part.at[slot, block((sib, diag, cp)[which])]
        dst = rs_cp.at[c] if which == 2 else rs_sib.at[which, c]
        target = cp if which == 2 else sib
        return pltpu.make_async_remote_copy(src, dst, rs_send.at[which, c], rs_recv.at[which, c], device_id={"ep": target}, device_id_type=MESH)

    def pp_copy(c):
        return pltpu.make_async_remote_copy(h_out.at[c], h_in.at[c], pp_send.at[c], pp_recv.at[c], device_id={"pp": lax.rem(stage + 1, stages)}, device_id_type=MESH)

    def bc_copy(c, target):
        return pltpu.make_async_remote_copy(out_ref.at[c], out_ref.at[c], bc_send.at[target, c], bc_recv.at[c], device_id={"pp": target}, device_id_type=MESH)

    lane = lax.broadcasted_iota(jnp.int32, (rows, 128), 1)
    low_half = lane < 64
    first_part = lax.rem(lane, 64) < 32
    own_head = lax.rem(lax.broadcasted_iota(jnp.int32, (16, 128), 1), 8) == lax.broadcasted_iota(jnp.int32, (16, 128), 0) // 2

    slot_of_lane = (lax.broadcasted_iota(jnp.int32, (1, 128), 1) // 8).astype(F32)

    def rope(vals, cos, sin):
        turned = jnp.where(first_part, pltpu.roll(vals, 96, 1), pltpu.roll(vals, 32, 1))
        return rounded(vals * cos + turned * sin)

    def project(c):

        @pl.when(stage > 0)
        def _():
            pp_copy(c).wait_recv()

        @pl.when((stage == 0) & (c == 0))
        def _():
            hid_copy.wait()

        @pl.when(c == 0)
        def _():
            for copy in attn_w:
                copy.wait()

            @pl.loop(0, 8)
            def _(j):
                for copy in expert_w(j):
                    copy.start()

        @pl.when(c + 1 < chunks)
        def _():
            for copy in kv_copies(c + 1):
                copy.start()

        for m in range(rows // 16):
            at = lax.broadcasted_iota(jnp.int32, pos_ref.shape, 1) == c * (rows // 16) + m
            col = jnp.sum(jnp.where(at, pos_ref[...], 0).astype(F32), axis=1, keepdims=True)
            pos_col[m * 16:(m + 1) * 16, :] = jnp.broadcast_to(col, (16, 128))
        where_pos = pos_col[...]
        cos = jnp.zeros((rows, 128), F32)
        sin = jnp.zeros((rows, 128), F32)
        for p in range(16):
            here = where_pos == p + 1.0
            cos = jnp.where(here, rot_ref[0, p:p + 1, :], cos)
            sin = jnp.where(here, rot_ref[1, p:p + 1, :], sin)
        normed = rms(h_in[c].astype(F32), ag_ref[...])
        query = rounded(dot(normed, wq[...]))
        key = rounded(dot(normed, wk[...]))
        value = rounded(dot(normed, wv[...]))
        for j in range(8):
            piece = rope(query[:, j * 128:(j + 1) * 128], cos, sin)
            q2[pl.ds(2 * j, rows, stride=16), :] = piece
            q2[pl.ds(2 * j + 1, rows, stride=16), :] = pltpu.roll(piece, 64, 1)
        for which, full in ((0, key), (1, value)):
            spread = (k2, v2)[which]
            for j in range(4):
                piece = full[:, j * 128:(j + 1) * 128]
                if which == 0:
                    piece = rope(piece, cos, sin)
                other = pltpu.roll(piece, 64, 1)
                kn[which, pl.ds(2 * j, rows, stride=8), :] = piece
                kn[which, pl.ds(2 * j + 1, rows, stride=8), :] = other
                spread[pl.ds(4 * j, rows, stride=16), :] = piece
                spread[pl.ds(4 * j + 1, rows, stride=16), :] = piece
                spread[pl.ds(4 * j + 2, rows, stride=16), :] = other
                spread[pl.ds(4 * j + 3, rows, stride=16), :] = other
        new_span = pl.ds(pl.multiple_of(c * rows * 8, rows * 8), rows * 8)
        ko_ref[new_span, :] = kn[0, :, :64].astype(BF16)
        vo_ref[new_span, :] = kn[1, :, :64].astype(BF16)

    def attend(c):
        slot = lax.rem(c, 2)
        for copy in kv_copies(c):
            copy.wait()

        @pl.loop(0, rows // 8, unroll=UNROLL)
        def _(g):
            heads = pl.ds(pl.multiple_of(g * 128, 128), 128)
            q_f32 = q2[heads, :64]
            q_bf = q_f32.astype(BF16)
            scores = []
            for b in range(8):
                keys = kbuf[slot, pl.ds(pl.multiple_of((g * 8 + b) * 128, 128), 128), :]
                valid = pos_col[pl.ds(g * 8 + b, 1), :] > slot_of_lane
                one = dot_t(q_bf[b * 16:(b + 1) * 16], keys) * 0.125
                scores.append(jnp.where(own_head & valid, one, -jnp.inf))
            score = jnp.concatenate(scores, axis=0)
            self_score = jnp.sum(q_f32 * k2[heads, :64], axis=1, keepdims=True) * 0.125
            top = jnp.maximum(jnp.max(score, axis=1, keepdims=True), self_score)
            weight = jnp.exp(score - top)
            self_w = jnp.exp(self_score - top)
            total = jnp.sum(weight, axis=1, keepdims=True) + self_w
            weight = (weight / total).astype(BF16)
            self_w = rounded(self_w / total)
            outs = []
            for b in range(8):
                vals = vbuf[slot, pl.ds(pl.multiple_of((g * 8 + b) * 128, 128), 128), :]
                outs.append(dot(weight[b * 16:(b + 1) * 16], vals))
            mixed = jnp.concatenate(outs, axis=0) + self_w * v2[heads, :64]
            o2[heads, :64] = mixed

        pieces = []
        for j in range(8):
            even = o2[pl.ds(2 * j, rows, stride=16), :]
            odd = o2[pl.ds(2 * j + 1, rows, stride=16), :]
            pieces.append(jnp.where(low_half, even, pltpu.roll(odd, 64, 1)).astype(BF16))
        attn_out = jnp.concatenate(pieces, axis=1)
        mid = (h_in[c].astype(F32) + dot(attn_out, wo[...])).astype(BF16)
        h_mid[c] = mid
        n_all[c, block(me), :] = rms(mid.astype(F32), mg_ref[...])
        ag_copy(1, c).start()
        ag_copy(0, c).start()

    def gates(c):
        logits = dot_t(n_all[c], wr_ref[...])
        lane32 = lax.broadcasted_iota(jnp.int32, (16, 32), 1)
        flags = []
        for src in range(4):
            for m in range(rows // 16):
                at = lax.broadcasted_iota(jnp.int32, (16, 128), 1) == c * (rows // 16) + m
                low = jnp.sum(jnp.where(at, bits[src, 0], 0.0), axis=1, keepdims=True)
                high = jnp.sum(jnp.where(at, bits[src, 1], 0.0), axis=1, keepdims=True)
                halves = jnp.where(lane32 < 16, low, high).astype(jnp.int32)
                flags.append(lax.shift_right_logical(halves, lax.rem(lane32, 16)) & 1)
        chosen = jnp.concatenate(flags, axis=0) > 0
        logits = jnp.where(chosen, logits, -jnp.inf)
        grown = jnp.exp(logits - jnp.max(logits, axis=1, keepdims=True))
        share = grown / jnp.sum(grown, axis=1, keepdims=True)
        expert_lane = lax.broadcasted_iota(jnp.int32, (every, 32), 1)
        for j in range(8):
            col = jnp.sum(jnp.where(expert_lane == me * 8 + j, share, 0.0), axis=1, keepdims=True)
            coef[j] = jnp.broadcast_to(col, (every, 128))

    def gate_up(c, j, act):
        for f in range(2):
            here = slice(f * 256, (f + 1) * 256)
            gate_h = dot(n_all[c], wg[j, :, here])
            up_h = dot(n_all[c], wu[j, :, here])
            act[:, here] = (gate_h / (1.0 + jnp.exp(-gate_h)) * up_h).astype(BF16)

    def down(c, j, act):
        slot = lax.rem(c, 2)
        scale = coef[j]
        for f in range(4):
            term = dot(act[...], wd[j, :, f * 256:(f + 1) * 256])
            for v in range(2):
                here = slice(f * 256 + v * 128, f * 256 + (v + 1) * 128)
                part[slot, :, here] += rounded(scale * term[:, v * 128:(v + 1) * 128])

    def expert_pairs(c, first, count):
        @pl.loop(first, first + count)
        def _(t):
            gate_up(c, 2 * t + 1, act_odd)
            down(c, 2 * t, act_even)
            gate_up(c, 2 * t + 2, act_even)
            down(c, 2 * t + 1, act_odd)

    def loading_experts(c):
        @pl.loop(0, 8)
        def _(j):
            for copy in expert_w(j):
                copy.wait()
            gate_up(c, j, act_even)
            down(c, j, act_even)

    def chip_sum(c):
        slot = lax.rem(c, 2)
        rs_copy(0, c).wait_recv()
        rs_copy(1, c).wait_recv()
        part[slot, block(cp), :] += rs_sib[1, c]
        rs_copy(2, c).start()

    def finish(c):
        slot = lax.rem(c, 2)
        rs_copy(2, c).wait_recv()
        total = part[slot, block(me), :] + rs_sib[0, c] + rs_cp[c]
        result = (h_mid[c].astype(F32) + rounded(total)).astype(BF16)

        @pl.when(stage < last)
        def _():
            h_out[c] = result
            pp_copy(c).start()

        @pl.when(stage == last)
        def _():
            out_ref[c] = rms(result.astype(F32), fg_ref[...].astype(F32).reshape(1, -1))
            for target in range(last):
                bc_copy(c, target).start()

    @pl.loop(0, chunks + 2)
    def _(i):
        @pl.when(i < chunks)
        def _():
            project(i)

        @pl.when(i >= 2)
        def _():
            chip_sum(i - 2)

        has_moe = (i >= 1) & (i <= chunks)

        @pl.when(has_moe)
        def _():
            ag_copy(1, i - 1).wait_recv()
            ag_copy(2, i - 1).start()

        @pl.when(i < chunks)
        def _():
            attend(i)

        @pl.when(has_moe)
        def _():
            c = i - 1

            @pl.when(c == 0)
            def _():
                for which in range(3):
                    bit_copy(which).wait_recv()

            @pl.when(c >= 2)
            def _():
                for which in range(3):
                    rs_copy(which, c - 2).wait_send()

            part[lax.rem(c, 2)] = jnp.zeros((every, part.shape[2]), F32)
            ag_copy(0, c).wait_recv()
            ag_copy(2, c).wait_recv()
            gates(c)

            @pl.when(c == 0)
            def _():
                loading_experts(c)

            @pl.when(c > 0)
            def _():
                gate_up(c, 0, act_even)
                expert_pairs(c, 0, 2)

        @pl.when(i >= 2)
        def _():
            finish(i - 2)

        @pl.when(has_moe)
        def _():
            c = i - 1

            @pl.when(c > 0)
            def _():
                expert_pairs(c, 2, 1)
                gate_up(c, 7, act_odd)
                down(c, 6, act_even)
                down(c, 7, act_odd)

            rs_copy(1, c).start()
            rs_copy(0, c).start()

    for which in range(3):
        bit_copy(which).wait_send()
        rs_copy(which, chunks - 2).wait_send()
        rs_copy(which, chunks - 1).wait_send()

    @pl.loop(0, chunks)
    def _(c):
        for which in range(3):
            ag_copy(which, c).wait_send()

        @pl.when(stage < last)
        def _():
            pp_copy(c).wait_send()
            bc_copy(c, 0).wait_recv()

        @pl.when(stage == last)
        def _():
            for target in range(last):
                bc_copy(c, target).wait_send()


def place_kernel(a_ref, b_ref, c_ref, a_out, b_out, c_out, sems):
    copies = [pltpu.make_async_copy(src, dst, sems.at[i]) for i, (src, dst) in enumerate(((a_ref, a_out), (b_ref, b_out), (c_ref, c_out)))]
    for copy in copies:
        copy.start()
    for copy in copies:
        copy.wait()


def place(arrays):
    return pl.pallas_call(
        place_kernel,
        out_shape=tuple(jax.ShapeDtypeStruct(arr.shape, arr.dtype) for arr in arrays),
        in_specs=[pl.BlockSpec(memory_space=pltpu.VMEM)] * 3,
        out_specs=(pl.BlockSpec(memory_space=pl.ANY),) * 3,
        scratch_shapes=[pltpu.SemaphoreType.DMA((3,))],
    )(*arrays)


def run_stack(cfg, hidden, k_rows, v_rows, weights, rotation, positions, ids, gains, router):
    chunks, rows, stages = cfg
    every = 4 * rows
    width = hidden.shape[-1]
    w_q, w_k, w_v, w_o, w_g, w_u, w_d = weights
    vmem = pl.BlockSpec(memory_space=pltpu.VMEM)
    hbm = pl.BlockSpec(memory_space=pl.ANY)
    dma = pltpu.SemaphoreType.DMA
    new_shape = jax.ShapeDtypeStruct((chunks * rows * 8, 64), BF16)
    return pl.pallas_call(
        functools.partial(stack_kernel, cfg),
        out_shape=(jax.ShapeDtypeStruct((chunks, rows, width), BF16), new_shape, new_shape),
        in_specs=[hbm] * 10 + [vmem] * 7,
        out_specs=(vmem, vmem, vmem),
        scratch_shapes=[
            pltpu.VMEM(w_q.shape, BF16),
            pltpu.VMEM(w_k.shape, BF16),
            pltpu.VMEM(w_v.shape, BF16),
            pltpu.VMEM(w_o.shape, BF16),
            pltpu.VMEM(w_g.shape, BF16),
            pltpu.VMEM(w_u.shape, BF16),
            pltpu.VMEM(w_d.shape, BF16),
            pltpu.VMEM((chunks, rows, width), BF16),
            pltpu.VMEM((chunks, rows, width), BF16),
            pltpu.VMEM((chunks, rows, width), BF16),
            pltpu.VMEM((chunks, every, width), BF16),
            pltpu.VMEM((2, every, width), F32),
            pltpu.VMEM((2, chunks, rows, width), F32),
            pltpu.VMEM((chunks, rows, width), F32),
            pltpu.VMEM((2, rows * 128, 64), BF16),
            pltpu.VMEM((2, rows * 128, 64), BF16),
            pltpu.VMEM((rows * 16, 128), F32),
            pltpu.VMEM((rows * 16, 128), F32),
            pltpu.VMEM((rows * 16, 128), F32),
            pltpu.VMEM((rows * 16, 128), F32),
            pltpu.VMEM((2, rows * 8, 128), F32),
            pltpu.VMEM((every, w_g.shape[2]), BF16),
            pltpu.VMEM((every, w_g.shape[2]), BF16),
            pltpu.VMEM((8, every, 128), F32),
            pltpu.VMEM((rows, 128), F32),
            pltpu.VMEM((4, 2, 16, 128), F32),
            dma((28,)),
            dma((2, 2)),
            dma,
            dma((3,)),
            dma((3,)),
            dma((3, chunks)),
            dma((3, chunks)),
            dma((3, chunks)),
            dma((3, chunks)),
            dma((chunks,)),
            dma((chunks,)),
            dma((3, chunks)),
            dma((chunks,)),
        ],
        compiler_params=pltpu.CompilerParams(collective_id=0, has_side_effects=True, vmem_limit_bytes=67043328),
    )(hidden, k_rows, v_rows, w_q, w_k, w_v, w_o, w_g, w_u, w_d, rotation, positions, ids, *gains, router)


def solution(mesh):
    stages = mesh.shape["pp"]
    rows_spec = ("dp", "ep")
    three_dim = P("pp", None, None)
    two_dim = P("pp", None)
    expert_spec = P("pp", "ep", None, None)
    cache_spec = P("pp", None, rows_spec, None, None, None)
    new_spec = P("pp", None, rows_spec, None, None)
    in_specs = (P(None, rows_spec, None), P(None, rows_spec), cache_spec, cache_spec, P("pp", None, rows_spec, None), three_dim, three_dim, three_dim, three_dim, two_dim, two_dim, three_dim, expert_spec, expert_spec, expert_spec, P(None))
    out_specs = (P(None, rows_spec, None), new_spec, new_spec)

    def device_fn(hidden_in, seq_pos, k_cache, v_cache, expert_ids, w_query, w_key, w_value, w_out, attn_gain, mlp_gain, w_router, w_gate, w_up, w_down, final_gain):
        micro, tokens, width = hidden_in.shape
        rows = MICRO_PER_CHUNK * tokens
        chunks = micro // MICRO_PER_CHUNK
        half = 32
        inv_freq = (THETA ** (-np.arange(half) / half)).astype(np.float32)
        angles = (np.arange(1, 17, dtype=np.float32)[:, None] * np.tile(inv_freq, 4)[None, :]).astype(np.float32)
        sign = np.where(np.arange(128) % 64 < 32, -1.0, 1.0)
        rotation = jnp.asarray(np.stack([np.cos(angles), sign * np.sin(angles)]).astype(np.float32))
        gains = (attn_gain, mlp_gain, final_gain)
        weights = (w_query[0], w_key[0], w_value[0], w_out[0], w_gate[0], w_up[0], w_down[0])
        out, k_new, v_new = place(run_stack((chunks, rows, stages), hidden_in.reshape(chunks, rows, width), k_cache.reshape(-1, 64), v_cache.reshape(-1, 64), weights, rotation, seq_pos.T, expert_ids[0].transpose(1, 2, 0), gains, w_router[0].T))
        new_shape = k_cache.shape[:3] + k_cache.shape[4:]
        return out.reshape(hidden_in.shape), k_new.reshape(new_shape), v_new.reshape(new_shape)

    return jax.shard_map(device_fn, mesh=mesh, in_specs=in_specs, out_specs=out_specs, check_vma=False)
```

```python
import functools

import jax
import jax.numpy as jnp
import numpy as np
from jax import lax
from jax.experimental import pallas as pl
from jax.experimental.pallas import tpu as pltpu
from jax.sharding import PartitionSpec as P

THETA = 1000000.0
EPS = 1e-05
MICRO_PER_CHUNK = 2
MESH = pl.DeviceIdType.MESH
F32 = jnp.float32
BF16 = jnp.bfloat16


def rms(vals, gain):
    inv = lax.rsqrt(jnp.mean(vals * vals, axis=-1, keepdims=True) + EPS)
    return (vals * inv * gain.astype(F32)).astype(BF16)


def dot(lhs, rhs):
    return jnp.dot(lhs, rhs, preferred_element_type=F32)


def dot_t(lhs, rhs):
    return lax.dot_general(lhs, rhs, (((1,), (1,)), ((), ())), preferred_element_type=F32)


def rounded(vals):
    return vals.astype(BF16).astype(F32)


def stack_kernel(cfg, hid_hbm, k_hbm, v_hbm, wq_hbm, wk_hbm, wv_hbm, wo_hbm, wg_hbm, wu_hbm, wd_hbm, rot_ref, pos_ref, ids_ref, ag_ref, mg_ref, fg_ref, wr_ref, out_ref, ko_ref, vo_ref, wq, wk, wv, wo, wg, wu, wd, h_in, h_mid, h_out, n_all, part, rs_sib, rs_cp, kbuf, vbuf, q2, k2, v2, o2, kn, act_even, act_odd, coef, pos_col, bits, w_sem, kv_sem, hid_sem, bit_send, bit_recv, ag_send, ag_recv, rs_send, rs_recv, pp_send, pp_recv, bc_send, bc_recv):
    chunks, rows, stages = cfg
    every = 4 * rows
    stage = lax.axis_index("pp")
    me = lax.axis_index("ep")
    sib = me + 1 - 2 * lax.rem(me, 2)
    cp = lax.rem(me + 2, 4)
    diag = lax.rem(sib + 2, 4)
    last = stages - 1

    def block(dev):
        return pl.ds(pl.multiple_of(dev * rows, rows), rows)

    def guard(steady, pred):
        return (lambda fn: fn()) if steady else pl.when(pred)

    def repeat(steady, first, count):
        def run(fn):
            if not steady:
                pl.loop(first, first + count)(fn)
            else:
                for step in range(first, first + count):
                    fn(step)

        return run

    attn_w = [pltpu.make_async_copy(src, dst, w_sem.at[i]) for i, (src, dst) in enumerate(((wq_hbm, wq), (wk_hbm, wk), (wv_hbm, wv), (wo_hbm, wo)))]
    def expert_w(j):
        return [pltpu.make_async_copy(src.at[j], dst.at[j], w_sem.at[4 + which * 8 + j]) for which, (src, dst) in enumerate(((wg_hbm, wg), (wu_hbm, wu), (wd_hbm, wd)))]

    def kv_copies(c):
        slot = lax.rem(c, 2)
        span = pl.ds(pl.multiple_of(c * rows * 128, rows * 128), rows * 128)
        return (pltpu.make_async_copy(k_hbm.at[span], kbuf.at[slot], kv_sem.at[0, slot]), pltpu.make_async_copy(v_hbm.at[span], vbuf.at[slot], kv_sem.at[1, slot]))

    hid_copy = pltpu.make_async_copy(hid_hbm, h_in, hid_sem)

    @pl.when(stage == 0)
    def _():
        hid_copy.start()

    for copy in attn_w:
        copy.start()
    for copy in kv_copies(0):
        copy.start()

    barrier = pltpu.get_barrier_semaphore()
    pl.semaphore_signal(barrier, inc=1, device_id={"ep": sib}, device_id_type=MESH)
    pl.semaphore_signal(barrier, inc=1, device_id={"ep": cp}, device_id_type=MESH)
    pl.semaphore_signal(barrier, inc=1, device_id={"ep": diag}, device_id_type=MESH)
    for step in range(1, stages):
        pl.semaphore_signal(barrier, inc=1, device_id={"pp": lax.rem(stage + step, stages)}, device_id_type=MESH)

    marks = jnp.zeros((16, ids_ref.shape[2]), jnp.int32)
    for k in range(8):
        marks = marks | lax.shift_left(jnp.int32(1), ids_ref[:, k, :])
    micro = marks.shape[1]
    bits[me, 0, :, :micro] = (marks & 65535).astype(F32)
    bits[me, 1, :, :micro] = (lax.shift_right_logical(marks, jnp.int32(16)) & 65535).astype(F32)
    pl.semaphore_wait(barrier, 3 + stages - 1)

    def bit_copy(which):
        return pltpu.make_async_remote_copy(bits.at[me], bits.at[me], bit_send.at[which], bit_recv.at[which], device_id={"ep": (sib, cp, diag)[which]}, device_id_type=MESH)

    for which in range(3):
        bit_copy(which).start()

    def ag_copy(which, c):
        src = n_all.at[c, block(cp if which == 2 else me)]
        target = cp if which == 1 else sib
        return pltpu.make_async_remote_copy(src, src, ag_send.at[which, c], ag_recv.at[which, c], device_id={"ep": target}, device_id_type=MESH)

    def rs_copy(which, c):
        slot = lax.rem(c, 2)
        src = part.at[slot, block((sib, diag, cp)[which])]
        dst = rs_cp.at[c] if which == 2 else rs_sib.at[which, c]
        target = cp if which == 2 else sib
        return pltpu.make_async_remote_copy(src, dst, rs_send.at[which, c], rs_recv.at[which, c], device_id={"ep": target}, device_id_type=MESH)

    def pp_copy(c):
        return pltpu.make_async_remote_copy(h_out.at[c], h_in.at[c], pp_send.at[c], pp_recv.at[c], device_id={"pp": lax.rem(stage + 1, stages)}, device_id_type=MESH)

    def bc_copy(c, target):
        return pltpu.make_async_remote_copy(out_ref.at[c], out_ref.at[c], bc_send.at[target, c], bc_recv.at[c], device_id={"pp": target}, device_id_type=MESH)

    lane = lax.broadcasted_iota(jnp.int32, (rows, 128), 1)
    low_half = lane < 64
    first_part = lax.rem(lane, 64) < 32
    own_head = lax.rem(lax.broadcasted_iota(jnp.int32, (16, 128), 1), 8) == lax.broadcasted_iota(jnp.int32, (16, 128), 0) // 2

    slot_of_lane = (lax.broadcasted_iota(jnp.int32, (1, 128), 1) // 8).astype(F32)

    def rope(vals, cos, sin):
        turned = jnp.where(first_part, pltpu.roll(vals, 96, 1), pltpu.roll(vals, 32, 1))
        return rounded(vals * cos + turned * sin)

    def project(c, steady):

        @pl.when(stage > 0)
        def _():
            pp_copy(c).wait_recv()

        if not steady:
            @pl.when((stage == 0) & (c == 0))
            def _():
                hid_copy.wait()

            @pl.when(c == 0)
            def _():
                for copy in attn_w:
                    copy.wait()

                @pl.loop(0, 8)
                def _(j):
                    for copy in expert_w(j):
                        copy.start()

        @pl.when(c + 1 < chunks)
        def _():
            for copy in kv_copies(c + 1):
                copy.start()

        for m in range(rows // 16):
            at = lax.broadcasted_iota(jnp.int32, pos_ref.shape, 1) == c * (rows // 16) + m
            col = jnp.sum(jnp.where(at, pos_ref[...], 0).astype(F32), axis=1, keepdims=True)
            pos_col[m * 16:(m + 1) * 16, :] = jnp.broadcast_to(col, (16, 128))
        where_pos = pos_col[...]
        cos = jnp.zeros((rows, 128), F32)
        sin = jnp.zeros((rows, 128), F32)
        for p in range(16):
            here = where_pos == p + 1.0
            cos = jnp.where(here, rot_ref[0, p:p + 1, :], cos)
            sin = jnp.where(here, rot_ref[1, p:p + 1, :], sin)
        normed = rms(h_in[c].astype(F32), ag_ref[...])
        query = rounded(dot(normed, wq[...]))
        key = rounded(dot(normed, wk[...]))
        value = rounded(dot(normed, wv[...]))
        for j in range(8):
            piece = rope(query[:, j * 128:(j + 1) * 128], cos, sin)
            q2[pl.ds(2 * j, rows, stride=16), :] = piece
            q2[pl.ds(2 * j + 1, rows, stride=16), :] = pltpu.roll(piece, 64, 1)
        for which, full in ((0, key), (1, value)):
            spread = (k2, v2)[which]
            for j in range(4):
                piece = full[:, j * 128:(j + 1) * 128]
                if which == 0:
                    piece = rope(piece, cos, sin)
                other = pltpu.roll(piece, 64, 1)
                kn[which, pl.ds(2 * j, rows, stride=8), :] = piece
                kn[which, pl.ds(2 * j + 1, rows, stride=8), :] = other
                spread[pl.ds(4 * j, rows, stride=16), :] = piece
                spread[pl.ds(4 * j + 1, rows, stride=16), :] = piece
                spread[pl.ds(4 * j + 2, rows, stride=16), :] = other
                spread[pl.ds(4 * j + 3, rows, stride=16), :] = other
        new_span = pl.ds(pl.multiple_of(c * rows * 8, rows * 8), rows * 8)
        ko_ref[new_span, :] = kn[0, :, :64].astype(BF16)
        vo_ref[new_span, :] = kn[1, :, :64].astype(BF16)

    def attend(c, steady):
        slot = lax.rem(c, 2)
        for copy in kv_copies(c):
            copy.wait()

        @repeat(steady, 0, rows // 8)
        def _(g):
            heads = pl.ds(g * 128 if steady else pl.multiple_of(g * 128, 128), 128)
            q_f32 = q2[heads, :64]
            q_bf = q_f32.astype(BF16)
            scores = []
            for b in range(8):
                keys = kbuf[slot, pl.ds((g * 8 + b) * 128 if steady else pl.multiple_of((g * 8 + b) * 128, 128), 128), :]
                valid = pos_col[pl.ds(g * 8 + b, 1), :] > slot_of_lane
                one = dot_t(q_bf[b * 16:(b + 1) * 16], keys) * 0.125
                scores.append(jnp.where(own_head & valid, one, -jnp.inf))
            score = jnp.concatenate(scores, axis=0)
            self_score = jnp.sum(q_f32 * k2[heads, :64], axis=1, keepdims=True) * 0.125
            top = jnp.maximum(jnp.max(score, axis=1, keepdims=True), self_score)
            weight = jnp.exp(score - top)
            self_w = jnp.exp(self_score - top)
            total = jnp.sum(weight, axis=1, keepdims=True) + self_w
            weight = (weight / total).astype(BF16)
            self_w = rounded(self_w / total)
            outs = []
            for b in range(8):
                vals = vbuf[slot, pl.ds((g * 8 + b) * 128 if steady else pl.multiple_of((g * 8 + b) * 128, 128), 128), :]
                outs.append(dot(weight[b * 16:(b + 1) * 16], vals))
            mixed = jnp.concatenate(outs, axis=0) + self_w * v2[heads, :64]
            o2[heads, :64] = mixed

        pieces = []
        for j in range(8):
            even = o2[pl.ds(2 * j, rows, stride=16), :]
            odd = o2[pl.ds(2 * j + 1, rows, stride=16), :]
            pieces.append(jnp.where(low_half, even, pltpu.roll(odd, 64, 1)).astype(BF16))
        attn_out = jnp.concatenate(pieces, axis=1)
        mid = (h_in[c].astype(F32) + dot(attn_out, wo[...])).astype(BF16)
        h_mid[c] = mid
        n_all[c, block(me), :] = rms(mid.astype(F32), mg_ref[...])
        ag_copy(1, c).start()
        ag_copy(0, c).start()

    def gates(c):
        logits = dot_t(n_all[c], wr_ref[...])
        lane32 = lax.broadcasted_iota(jnp.int32, (16, 32), 1)
        flags = []
        for src in range(4):
            for m in range(rows // 16):
                at = lax.broadcasted_iota(jnp.int32, (16, 128), 1) == c * (rows // 16) + m
                low = jnp.sum(jnp.where(at, bits[src, 0], 0.0), axis=1, keepdims=True)
                high = jnp.sum(jnp.where(at, bits[src, 1], 0.0), axis=1, keepdims=True)
                halves = jnp.where(lane32 < 16, low, high).astype(jnp.int32)
                flags.append(lax.shift_right_logical(halves, lax.rem(lane32, 16)) & 1)
        chosen = jnp.concatenate(flags, axis=0) > 0
        logits = jnp.where(chosen, logits, -jnp.inf)
        grown = jnp.exp(logits - jnp.max(logits, axis=1, keepdims=True))
        share = grown / jnp.sum(grown, axis=1, keepdims=True)
        expert_lane = lax.broadcasted_iota(jnp.int32, (every, 32), 1)
        for j in range(8):
            col = jnp.sum(jnp.where(expert_lane == me * 8 + j, share, 0.0), axis=1, keepdims=True)
            coef[j] = jnp.broadcast_to(col, (every, 128))

    def gate_up(c, j, act):
        for f in range(2):
            here = slice(f * 256, (f + 1) * 256)
            gate_h = dot(n_all[c], wg[j, :, here])
            up_h = dot(n_all[c], wu[j, :, here])
            act[:, here] = (gate_h / (1.0 + jnp.exp(-gate_h)) * up_h).astype(BF16)

    def down(c, j, act):
        slot = lax.rem(c, 2)
        scale = coef[j]
        for f in range(4):
            term = dot(act[...], wd[j, :, f * 256:(f + 1) * 256])
            for v in range(2):
                here = slice(f * 256 + v * 128, f * 256 + (v + 1) * 128)
                part[slot, :, here] += rounded(scale * term[:, v * 128:(v + 1) * 128])

    def expert_pairs(c, first, count, steady):
        @repeat(steady, first, count)
        def _(t):
            gate_up(c, 2 * t + 1, act_odd)
            down(c, 2 * t, act_even)
            gate_up(c, 2 * t + 2, act_even)
            down(c, 2 * t + 1, act_odd)

    def loading_experts(c):
        @pl.loop(0, 8)
        def _(j):
            for copy in expert_w(j):
                copy.wait()
            gate_up(c, j, act_even)
            down(c, j, act_even)

    def chip_sum(c):
        slot = lax.rem(c, 2)
        rs_copy(0, c).wait_recv()
        rs_copy(1, c).wait_recv()
        part[slot, block(cp), :] += rs_sib[1, c]
        rs_copy(2, c).start()

    def finish(c):
        slot = lax.rem(c, 2)
        rs_copy(2, c).wait_recv()
        total = part[slot, block(me), :] + rs_sib[0, c] + rs_cp[c]
        result = (h_mid[c].astype(F32) + rounded(total)).astype(BF16)

        @pl.when(stage < last)
        def _():
            h_out[c] = result
            pp_copy(c).start()

        @pl.when(stage == last)
        def _():
            out_ref[c] = rms(result.astype(F32), fg_ref[...].astype(F32).reshape(1, -1))
            for target in range(last):
                bc_copy(c, target).start()

    def trip(i, steady):
        has_moe = (i >= 1) & (i <= chunks)

        @guard(steady, i < chunks)
        def _():
            project(i, steady)

        @guard(steady, i >= 2)
        def _():
            chip_sum(i - 2)

        @guard(steady, has_moe)
        def _():
            ag_copy(1, i - 1).wait_recv()
            ag_copy(2, i - 1).start()

        @guard(steady, i < chunks)
        def _():
            attend(i, steady)

        @guard(steady, has_moe)
        def _():
            c = i - 1
            if not steady:
                @pl.when(c == 0)
                def _():
                    for which in range(3):
                        bit_copy(which).wait_recv()

            @guard(steady, c >= 2)
            def _():
                for which in range(3):
                    rs_copy(which, c - 2).wait_send()

            part[lax.rem(c, 2)] = jnp.zeros((every, part.shape[2]), F32)
            ag_copy(0, c).wait_recv()
            ag_copy(2, c).wait_recv()
            gates(c)

            if not steady:
                @pl.when(c == 0)
                def _():
                    loading_experts(c)

            @guard(steady, c > 0)
            def _():
                gate_up(c, 0, act_even)
                expert_pairs(c, 0, 2, steady)

        @guard(steady, i >= 2)
        def _():
            finish(i - 2)

        @guard(steady, has_moe)
        def _():
            c = i - 1

            @guard(steady, c > 0)
            def _():
                expert_pairs(c, 2, 1, steady)
                gate_up(c, 7, act_odd)
                down(c, 6, act_even)
                down(c, 7, act_odd)

            rs_copy(1, c).start()
            rs_copy(0, c).start()

    @pl.loop(0, chunks + 2)
    def _(i):
        settled = (i >= 3) & (i < chunks)

        @pl.when(settled)
        def _():
            trip(i, True)

        @pl.when(jnp.logical_not(settled))
        def _():
            trip(i, False)

    for which in range(3):
        bit_copy(which).wait_send()
        rs_copy(which, chunks - 2).wait_send()
        rs_copy(which, chunks - 1).wait_send()

    @pl.loop(0, chunks)
    def _(c):
        for which in range(3):
            ag_copy(which, c).wait_send()

        @pl.when(stage < last)
        def _():
            pp_copy(c).wait_send()
            bc_copy(c, 0).wait_recv()

        @pl.when(stage == last)
        def _():
            for target in range(last):
                bc_copy(c, target).wait_send()


def place_kernel(a_ref, b_ref, c_ref, a_out, b_out, c_out, sems):
    copies = [pltpu.make_async_copy(src, dst, sems.at[i]) for i, (src, dst) in enumerate(((a_ref, a_out), (b_ref, b_out), (c_ref, c_out)))]
    for copy in copies:
        copy.start()
    for copy in copies:
        copy.wait()


def place(arrays):
    return pl.pallas_call(
        place_kernel,
        out_shape=tuple(jax.ShapeDtypeStruct(arr.shape, arr.dtype) for arr in arrays),
        in_specs=[pl.BlockSpec(memory_space=pltpu.VMEM)] * 3,
        out_specs=(pl.BlockSpec(memory_space=pl.ANY),) * 3,
        scratch_shapes=[pltpu.SemaphoreType.DMA((3,))],
    )(*arrays)


def run_stack(cfg, hidden, k_rows, v_rows, weights, rotation, positions, ids, gains, router):
    chunks, rows, stages = cfg
    every = 4 * rows
    width = hidden.shape[-1]
    w_q, w_k, w_v, w_o, w_g, w_u, w_d = weights
    vmem = pl.BlockSpec(memory_space=pltpu.VMEM)
    hbm = pl.BlockSpec(memory_space=pl.ANY)
    dma = pltpu.SemaphoreType.DMA
    new_shape = jax.ShapeDtypeStruct((chunks * rows * 8, 64), BF16)
    return pl.pallas_call(
        functools.partial(stack_kernel, cfg),
        out_shape=(jax.ShapeDtypeStruct((chunks, rows, width), BF16), new_shape, new_shape),
        in_specs=[hbm] * 10 + [vmem] * 7,
        out_specs=(vmem, vmem, vmem),
        scratch_shapes=[
            pltpu.VMEM(w_q.shape, BF16),
            pltpu.VMEM(w_k.shape, BF16),
            pltpu.VMEM(w_v.shape, BF16),
            pltpu.VMEM(w_o.shape, BF16),
            pltpu.VMEM(w_g.shape, BF16),
            pltpu.VMEM(w_u.shape, BF16),
            pltpu.VMEM(w_d.shape, BF16),
            pltpu.VMEM((chunks, rows, width), BF16),
            pltpu.VMEM((chunks, rows, width), BF16),
            pltpu.VMEM((chunks, rows, width), BF16),
            pltpu.VMEM((chunks, every, width), BF16),
            pltpu.VMEM((2, every, width), F32),
            pltpu.VMEM((2, chunks, rows, width), F32),
            pltpu.VMEM((chunks, rows, width), F32),
            pltpu.VMEM((2, rows * 128, 64), BF16),
            pltpu.VMEM((2, rows * 128, 64), BF16),
            pltpu.VMEM((rows * 16, 128), F32),
            pltpu.VMEM((rows * 16, 128), F32),
            pltpu.VMEM((rows * 16, 128), F32),
            pltpu.VMEM((rows * 16, 128), F32),
            pltpu.VMEM((2, rows * 8, 128), F32),
            pltpu.VMEM((every, w_g.shape[2]), BF16),
            pltpu.VMEM((every, w_g.shape[2]), BF16),
            pltpu.VMEM((8, every, 128), F32),
            pltpu.VMEM((rows, 128), F32),
            pltpu.VMEM((4, 2, 16, 128), F32),
            dma((28,)),
            dma((2, 2)),
            dma,
            dma((3,)),
            dma((3,)),
            dma((3, chunks)),
            dma((3, chunks)),
            dma((3, chunks)),
            dma((3, chunks)),
            dma((chunks,)),
            dma((chunks,)),
            dma((3, chunks)),
            dma((chunks,)),
        ],
        compiler_params=pltpu.CompilerParams(collective_id=0, has_side_effects=True, vmem_limit_bytes=67043328),
    )(hidden, k_rows, v_rows, w_q, w_k, w_v, w_o, w_g, w_u, w_d, rotation, positions, ids, *gains, router)


def solution(mesh):
    stages = mesh.shape["pp"]
    rows_spec = ("dp", "ep")
    three_dim = P("pp", None, None)
    two_dim = P("pp", None)
    expert_spec = P("pp", "ep", None, None)
    cache_spec = P("pp", None, rows_spec, None, None, None)
    new_spec = P("pp", None, rows_spec, None, None)
    in_specs = (P(None, rows_spec, None), P(None, rows_spec), cache_spec, cache_spec, P("pp", None, rows_spec, None), three_dim, three_dim, three_dim, three_dim, two_dim, two_dim, three_dim, expert_spec, expert_spec, expert_spec, P(None))
    out_specs = (P(None, rows_spec, None), new_spec, new_spec)

    def device_fn(hidden_in, seq_pos, k_cache, v_cache, expert_ids, w_query, w_key, w_value, w_out, attn_gain, mlp_gain, w_router, w_gate, w_up, w_down, final_gain):
        micro, tokens, width = hidden_in.shape
        rows = MICRO_PER_CHUNK * tokens
        chunks = micro // MICRO_PER_CHUNK
        half = 32
        inv_freq = (THETA ** (-np.arange(half) / half)).astype(np.float32)
        angles = (np.arange(1, 17, dtype=np.float32)[:, None] * np.tile(inv_freq, 4)[None, :]).astype(np.float32)
        sign = np.where(np.arange(128) % 64 < 32, -1.0, 1.0)
        rotation = jnp.asarray(np.stack([np.cos(angles), sign * np.sin(angles)]).astype(np.float32))
        gains = (attn_gain, mlp_gain, final_gain)
        weights = (w_query[0], w_key[0], w_value[0], w_out[0], w_gate[0], w_up[0], w_down[0])
        out, k_new, v_new = place(run_stack((chunks, rows, stages), hidden_in.reshape(chunks, rows, width), k_cache.reshape(-1, 64), v_cache.reshape(-1, 64), weights, rotation, seq_pos.T, expert_ids[0].transpose(1, 2, 0), gains, w_router[0].T))
        new_shape = k_cache.shape[:3] + k_cache.shape[4:]
        return out.reshape(hidden_in.shape), k_new.reshape(new_shape), v_new.reshape(new_shape)

    return jax.shard_map(device_fn, mesh=mesh, in_specs=in_specs, out_specs=out_specs, check_vma=False)
```
